256 devices in a mesh: batch: 2 (over core), neuron: 128 (over z, y, x).
Axes of the slice: x: 4, y: 4, z: 8, core: 2. Of those that a mesh axis runs over, the one named last changes fastest.
Arguments:
- images: bfloat16 [32, 65536], P('batch', 'neuron'), parts along dimension 0, may hold values from 0 to 32
- tile_weights: bfloat16 [2, 16384, 128, 128], P(None, 'neuron'), may hold values from -0.375 to 0.375
- tile_blocks: int32 [2, 16384, 2], P(None, 'neuron'), may hold values from 0 to 511, as said below
- tile_count: int32 [2, 128], P(None, 'neuron'), may hold values from 96 to 128, as said below
- bias: float32 [2, 65536], P(None, 'neuron'), may hold values from -48 to 48
Outputs:
- activity: bfloat16 [32, 65536], P('batch', 'neuron'), parts along dimension 0
The draws below stay inside these ranges and needn't reach their ends.
There are 2 independent parts, one for each index of `batch`. The reference program is written for one: setup_inputs(seed, part) draws one part's arguments, and reference() takes and returns one part's arrays. A program takes and returns all parts, laid end to end along the dimension named above; an argument that names none is the same for every part. Nothing has to cross between parts.
Inputs may be any that keep to these rules, and one draw needn't show every extreme that they name: Slots 0 to tile_count[l, d] - 1 of device d are live in layer l; in every layer one device has all 128 live. `tile_blocks`: entry [l, d * 128 + s, :] is the row block and column block of slot s of device d. Within one device and layer the column blocks are all different, and at most 2 of them lie among the 4 column blocks of any one neuron device; in every layer the column blocks of some neuron device get exactly 2 live slots from every device.
All inputs are finite; a program needn't handle non-finite values.
Results may differ from the reference program's by a relative error of at most 0.0033.
Values may be sent and summed in bfloat16 or wider, within the bound.
A program may use at most 64 MiB of HBM per device.

```python
import jax
import jax.numpy as jnp
from jax import lax

NEURONS = 65536
BLOCK = 128
LAYERS = 2
IMAGES = 16
TILES_DEV = 128
BLK_DEV = 4
SLOT_MOST = 2
N_NEURON = 128


def distinct_order(key, shape):
    scores = jax.random.randint(key, shape, 0, 65536) * shape[-1] + jnp.arange(shape[-1], dtype=jnp.int32)
    return jnp.argsort(scores, axis=-1, stable=True).astype(jnp.int32)


def draw_tile_blocks(key, part):
    base_key = jax.random.fold_in(key, 23)
    key_rows, key_owner, key_common, key_offset, key_shuffle = jax.random.split(base_key, 5)
    row_ids = jax.random.randint(key_rows, (LAYERS, N_NEURON, TILES_DEV), 0, NEURONS // BLOCK)
    owner_order = distinct_order(key_owner, (LAYERS, N_NEURON, N_NEURON))
    common = jax.random.randint(key_common, (LAYERS, 1, 1), 0, N_NEURON)
    slot_ids = jnp.arange(TILES_DEV, dtype=jnp.int32)
    groups = jnp.broadcast_to(slot_ids // SLOT_MOST, (LAYERS, N_NEURON, TILES_DEV))
    chosen = jnp.take_along_axis(owner_order, groups, axis=-1)
    owners = (chosen - owner_order[:, :, :1] + common) % N_NEURON
    offsets = jax.random.randint(key_offset, (LAYERS, N_NEURON, N_NEURON), 0, BLK_DEV)
    shifted = jnp.take_along_axis(offsets, groups, axis=-1)
    local_ids = (shifted + slot_ids % SLOT_MOST) % BLK_DEV
    col_ids = owners * BLK_DEV + local_ids
    tail_order = distinct_order(key_shuffle, (LAYERS, N_NEURON, TILES_DEV - SLOT_MOST))
    tail = jnp.take_along_axis(col_ids[:, :, SLOT_MOST:], tail_order, axis=-1)
    col_ids = jnp.concatenate([col_ids[:, :, :SLOT_MOST], tail], axis=-1)
    stacked = jnp.stack([row_ids, col_ids], axis=-1)
    return stacked.reshape(LAYERS, N_NEURON * TILES_DEV, 2).astype(jnp.int32)


def draw_tile_count(key, part):
    base_key = jax.random.fold_in(key, 11)
    key_first, key_busy = jax.random.split(base_key, 2)
    counts = jax.random.randint(key_first, (LAYERS, N_NEURON), TILES_DEV - TILES_DEV // 4, TILES_DEV + 1)
    busiest = jax.random.randint(key_busy, (LAYERS, 1), 0, N_NEURON)
    counts = jnp.where(jnp.arange(N_NEURON, dtype=jnp.int32)[None, :] == busiest, TILES_DEV, counts)
    return counts.astype(jnp.int32)


def steps_of(rng, extent, cuts, least, top_value):
    loudness, own = 1.0, jax.random.fold_in(rng, 6)
    for axis_at, parts in cuts:
        heights = jnp.exp(jax.random.uniform(jax.random.fold_in(own, axis_at), (parts,), jnp.float32, least / len(cuts), top_value / len(cuts)))
        loudness = loudness * jnp.repeat(heights, extent[axis_at] // parts).reshape([-1 if axis == axis_at else 1 for axis in range(len(extent))])
    return loudness


def gaussian(stream_key, extent, spread, reach, cuts=(), kind=jnp.bfloat16):
    values = spread * jax.random.normal(stream_key, extent, jnp.float32)
    if cuts:
        values = values * steps_of(stream_key, extent, cuts, -0.22, 0.18)
    return jnp.clip(values, -reach, reach).astype(kind)


def setup_inputs(seed: int = 0, part: int = 0) -> dict:
    key_list = jax.random.split(jax.random.key(seed), 6)
    own_keys = jax.random.split(jax.random.fold_in(key_list[5], part), 6)
    return {
        "images": jnp.clip(32.0 * jax.random.uniform(own_keys[0], (IMAGES, NEURONS), jnp.float32) ** steps_of(own_keys[0], (IMAGES, NEURONS), ((1, 128),), -0.2, 0.2), 0.0, 32.0).astype(jnp.bfloat16),
        "tile_weights": gaussian(key_list[1], (LAYERS, N_NEURON * TILES_DEV, BLOCK, BLOCK), (2 * BLOCK) ** -0.5, 0.375, ((1, 128),)),
        "tile_blocks": draw_tile_blocks(jax.random.fold_in(key_list[5], 71), part),
        "tile_count": draw_tile_count(jax.random.fold_in(key_list[5], 71), part),
        "bias": gaussian(key_list[4], (LAYERS, NEURONS), 8.0, 48.0, ((1, 128),), jnp.float32),
    }


CEILING = 32.0


def reference(images, tile_weights, tile_blocks, tile_count, bias):
    all_blocks = NEURONS // BLOCK
    activity = images
    for layer_index in range(LAYERS):
        block_view = activity.reshape(IMAGES, all_blocks, BLOCK).astype(jnp.float32)

        def device_terms(totals, pieces):
            weights, blocks, live_count = pieces
            picked = jnp.take(block_view, blocks[:, 0], axis=1)
            products = jnp.einsum("bsk,skn->sbn", picked, weights.astype(jnp.float32))
            usable = jnp.arange(TILES_DEV, dtype=jnp.int32) < live_count
            products = jnp.where(usable[:, None, None], products, jnp.zeros_like(products))
            return totals.at[blocks[:, 1]].add(products), live_count

        initial = jnp.zeros((all_blocks, IMAGES, BLOCK), jnp.float32)
        totals, unused = lax.scan(
            device_terms,
            initial,
            (
                tile_weights[layer_index].reshape(N_NEURON, TILES_DEV, BLOCK, BLOCK),
                tile_blocks[layer_index].reshape(N_NEURON, TILES_DEV, 2),
                tile_count[layer_index],
            ),
        )
        summed = jnp.transpose(totals, (1, 0, 2)).reshape(IMAGES, NEURONS)
        activity = jnp.clip(summed + bias[layer_index][None, :], 0.0, CEILING).astype(jnp.bfloat16)
    return activity
```

```python
import functools

import jax
import jax.numpy as jnp
from jax import lax
from jax.experimental import pallas as pl
from jax.experimental.pallas import tpu as pltpu
from jax.sharding import Mesh
from jax.sharding import PartitionSpec as P

AXES = ("neuron_0", "neuron_1", "neuron_2")
Z, Y, X = AXES
CEILING = 32.0
WEIGHT_TOP = 0.375
MESH = pl.DeviceIdType.MESH
LANES = 128


class Part:
    def __init__(self, order, sizes, base, width):
        self.order = order
        self.n1, self.n2, self.n3 = (sizes[a] for a in order)
        self.base = base
        self.width = width

    def start(self, c3, c2, c1):
        return self.base + ((c3 * self.n2 + c2) * self.n1 + c1) * self.width

    def messages(self):
        out = [("a", o) for o in range(1, self.n1)]
        out += [("b", o) for o in range(1, self.n2)]
        half = self.n2 // 2
        for step in range(1, self.n3 // 2 + 1):
            for rel in range(self.n2):
                for way in (1, -1):
                    if 2 * step == self.n3 and (rel < half) != (way == 1):
                        continue
                    out.append(("c", step, rel, way))
        return out


def gather_parts(sizes):
    total = sizes[Z] * sizes[Y] * sizes[X]
    return [
        Part((X, Y, Z), sizes, 0, 2),
        Part((Z, Y, X), sizes, 2 * total, 1),
        Part((Z, X, Y), sizes, 3 * total, 1),
    ]


def encode(value, scale):
    coded = value * lax.rsqrt(jnp.abs(value) + 1e-30) * scale
    return jnp.round(coded).astype(jnp.int32).astype(jnp.int16)


def decode(coded):
    value = coded.astype(jnp.int32).astype(jnp.float32)
    return value * jnp.abs(value)


def kernel(sizes, layers, slots, rows, images, weights, blocks, count, bias, out, *scratch):
    (acts, held, products, table, peer, stab, speer, x_out, x_in, x_out2, x_in2, x_own,
     y_out, y_in, y_out2, y_in2, y_own, z_out, z_in, z_own,
     ag_send, ag_recv, rs_send, rs_recv, tab_send, tab_recv, copy_sem) = scratch
    nz, ny, nx = sizes[Z], sizes[Y], sizes[X]
    me = {axis: lax.axis_index(axis) for axis in AXES}
    zh = nz // 2
    width = rows * 0 + LANES
    shift_x, shift_y = nx.bit_length() - 1, ny.bit_length() - 1
    total = nz * ny * nx
    top = WEIGHT_TOP * CEILING * width
    scale1 = 32700.0 / top ** 0.5
    scale2 = 32700.0 / (top * max(nx, ny)) ** 0.5
    scale3 = 32700.0 / (top * nx * ny) ** 0.5
    back1, back2, back3 = 1 / scale1**2, 1 / scale2**2, 1 / scale3**2

    def other(axis, step):
        return lax.rem(me[axis] + step + sizes[axis], sizes[axis])

    barrier = pltpu.get_barrier_semaphore()
    partners = [(axis, o) for axis in AXES for o in range(1, sizes[axis])]
    for axis, o in partners:
        pl.semaphore_signal(barrier, inc=1, device_id={axis: other(axis, o)}, device_id_type=MESH)

    weight_copies = [
        pltpu.make_async_copy(weights.at[l], held.at[l], copy_sem.at[l]) for l in range(layers)
    ]
    for copy in weight_copies:
        copy.start()

    parts = gather_parts(sizes)

    def own_start(part):
        return part.start(me[part.order[2]], me[part.order[1]], me[part.order[0]])

    def put_acts(layer, j, value):
        if j < 2:
            acts[layer, own_start(parts[0]) + j] = value
        else:
            acts[layer, own_start(parts[j - 1])] = value

    for j in range(4):
        put_acts(0, j, images[:, j * LANES : (j + 1) * LANES])

    lane = lax.broadcasted_iota(jnp.int32, (1, LANES), 1)
    slot = lax.broadcasted_iota(jnp.int32, (LANES, LANES), 0)
    flat = jnp.concatenate(
        [blocks[0], blocks[1], jnp.zeros((4, LANES), jnp.int32)], axis=0
    )
    upright = jnp.transpose(flat)
    dx = lane & (nx - 1)
    dy = (lane >> shift_x) & (ny - 1)
    dz = lane >> (shift_x + shift_y)
    second = jnp.where((dz & 1) == 0, dy, dx)
    place = (second * zh + (dz >> 1)) * 2
    blank = (jnp.where((dz & 1) == 0, ny, nx)) * zh * 2
    for l in range(layers):
        r = blocks[l, 0:1, :]
        j = r & 3
        rx = (r >> 2) & (nx - 1)
        ry = (r >> (2 + shift_x)) & (ny - 1)
        rz = r >> (2 + shift_x + shift_y)
        spot = jnp.where(
            j < 2,
            parts[0].start(rz, ry, rx) + j,
            jnp.where(j == 2, parts[1].start(rx, ry, rz), parts[2].start(ry, rx, rz)),
        )
        table[l : l + 1, :] = spot
        key = jnp.where(slot < count[0, l], slot + 1, 0)
        col = upright[:, 2 * l + 1 : 2 * l + 2]
        before = jnp.zeros((1, LANES), jnp.int32)
        ranked = [jnp.zeros((1, LANES), jnp.int32) for _ in range(2)]
        for j in range(4):
            found = jnp.sum(jnp.where(col == lane * 4 + j, key, 0), axis=0, keepdims=True)
            live = found > 0
            table[8 + 4 * l + j : 9 + 4 * l + j, :] = jnp.where(live, found - 1, slots)
            table[16 + 4 * l + j : 17 + 4 * l + j, :] = jnp.where(live, place + before, blank)
            for k in range(2):
                ranked[k] = ranked[k] + jnp.where(before == k, found, 0)
            before = before + live.astype(jnp.int32)
        for k in range(2):
            table[2 + 2 * l + k : 3 + 2 * l + k, :] = jnp.where(
                ranked[k] > 0, ranked[k] - 1, slots
            )
    own_table = pltpu.make_async_copy(table.at[pl.ds(0, 16)], stab, copy_sem.at[layers])
    own_table.start()

    nothing = jnp.zeros((rows, LANES), jnp.int16)
    products[slots] = nothing
    for buffer in (x_in, y_in):
        for l in range(layers):
            for o in range(buffer.shape[1]):
                buffer[l, o, buffer.shape[2] - 1] = nothing

    pl.semaphore_wait(barrier, len(partners))

    started = []

    def send(src, dst, send_sem, recv_sem, axis, step):
        copy = pltpu.make_async_remote_copy(
            src_ref=src, dst_ref=dst, send_sem=send_sem, recv_sem=recv_sem,
            device_id={axis: other(axis, step)}, device_id_type=MESH,
        )
        copy.start()
        started.append(copy)

    def arrive(dst, send_sem, recv_sem, axis, step):
        pltpu.make_async_remote_copy(
            src_ref=dst, dst_ref=dst, send_sem=send_sem, recv_sem=recv_sem,
            device_id={axis: other(axis, step)}, device_id_type=MESH,
        ).wait_recv()

    def gather(layer):
        number = {}
        for at, part in enumerate(parts):
            for message in part.messages():
                number[(at, message)] = len(number)

        def range_of(part, message, coming):
            a1, a2, a3 = part.order
            kind = message[0]
            if kind == "a":
                first = part.start(me[a3], me[a2], other(a1, -message[1]) if coming else me[a1])
                return first, part.width, a1, message[1]
            if kind == "b":
                first = part.start(me[a3], other(a2, -message[1]) if coming else me[a2], 0)
                return first, part.n1 * part.width, a2, message[1]
            _, step, rel, way = message
            far = step if coming else step - 1
            first = part.start(other(a3, -way * far), other(a2, -rel), 0)
            return first, part.n1 * part.width, a3, way

        def go(at, message):
            n = number.get((at, message))
            if n is None:
                return
            first, size, axis, step = range_of(parts[at], message, False)
            view = acts.at[layer, pl.ds(first, size)]
            send(view, view, ag_send.at[layer, n], ag_recv.at[layer, n], axis, step)

        def come(at, message):
            n = number[(at, message)]
            first, size, axis, step = range_of(parts[at], message, True)
            view = acts.at[layer, pl.ds(first, size)]
            arrive(view, ag_send.at[layer, n], ag_recv.at[layer, n], axis, step)

        order = range(len(parts))
        for at in order:
            for way in (1, -1):
                pass
            for o in range(1, parts[at].n1):
                go(at, ("a", o))
        for at in order:
            for o in range(1, parts[at].n1):
                come(at, ("a", o))
            for way in (1, -1):
                go(at, ("c", 1, 0, way))
            for o in range(1, parts[at].n2):
                go(at, ("b", o))
        for rel in range(1, max(p.n2 for p in parts)):
            for at in order:
                if rel < parts[at].n2:
                    come(at, ("b", rel))
                    for way in (1, -1):
                        go(at, ("c", 1, rel, way))
        for step in range(1, max(p.n3 for p in parts) // 2 + 1):
            for rel in range(max(p.n2 for p in parts)):
                for at in order:
                    for way in (1, -1):
                        if (at, ("c", step, rel, way)) in number:
                            come(at, ("c", step, rel, way))
                            go(at, ("c", step + 1, rel, way))

    sets = [
        (0, X, Y, x_out, x_in, x_out2, x_in2, x_own),
        (1, Y, X, y_out, y_in, y_out2, y_in2, y_own),
    ]
    n_peer = [0, nx - 1]
    for par, a1, a2, *_ in sets:
        for o in range(1, sizes[a1]):
            n = n_peer[par] + o - 1
            send(table.at[pl.ds(16, 8)], peer.at[n], tab_send.at[n], tab_recv.at[n], a1, o)

    def device_of(par, zi, c1, c2):
        y, x = (c2, c1) if par == 0 else (c1, c2)
        return ((2 * zi + par) * ny + y) * nx + x

    def loop(length, body, unroll):
        unroll = min(unroll, length)

        @pl.loop(0, length // unroll)
        def _(at):
            for u in range(unroll):
                body(at * unroll + u)

    for layer in range(layers):
        gather(layer)
        if layer == 0:
            own_table.wait()
            for par, a1, a2, *_ in sets:
                for o in range(1, sizes[a1]):
                    n = n_peer[par] + o - 1
                    arrive(peer.at[n], tab_send.at[n], tab_recv.at[n], a1, o)
            peer_table = pltpu.make_async_copy(peer, speer, copy_sem.at[layers + 1])
            peer_table.start()
        weight_copies[layer].wait()

        def multiply(s):
            got = jnp.dot(
                acts[layer, stab[layer, s]], held[layer, s], preferred_element_type=jnp.float32
            )
            products[s] = encode(got, scale1)

        loop(slots, multiply, 16)
        if layer == 0:
            peer_table.wait()

        sem = 0
        first_sem = {}
        for o in range(1, max(nx, ny)):
            for par, a1, a2, out1, in1, *_ in sets:
                n1, n2 = sizes[a1], sizes[a2]
                if o >= n1:
                    continue
                target = other(a1, o)

                def pack(p):
                    q = p >> 1
                    d = device_of(par, q & (zh - 1), target, q // zh)
                    out1[layer, o - 1, p] = products[stab[2 + 2 * layer + (p & 1), d]]

                loop(n2 * zh * 2, pack, 8)
                first_sem[(par, o)] = sem
                send(
                    out1.at[layer, o - 1], in1.at[layer, o - 1, pl.ds(0, n2 * zh * 2)],
                    rs_send.at[layer, sem], rs_recv.at[layer, sem], a1, o,
                )
                sem += 1

        second_sem = {}
        for par, a1, a2, out1, in1, out2, in2, own in sets:
            n1, n2 = sizes[a1], sizes[a2]
            for o in range(1, n1):
                at = first_sem[(par, o)]
                arrive(
                    in1.at[layer, o - 1, pl.ds(0, n2 * zh * 2)],
                    rs_send.at[layer, at], rs_recv.at[layer, at], a1, o,
                )
            for o2 in list(range(1, n2)) + [0]:
                target = other(a2, o2)

                def add(q):
                    j = q & 3
                    d = device_of(par, q >> 2, me[a1], target)
                    acc = decode(products[stab[8 + 4 * layer + j, d]])
                    for o in range(1, n1):
                        n = n_peer[par] + o - 1
                        acc = acc + decode(in1[layer, o - 1, speer[n, 4 * layer + j, d]])
                    acc = acc * back1
                    if o2:
                        out2[layer, o2 - 1, q] = encode(acc, scale2)
                    else:
                        own[q] = acc

                loop(zh * 4, add, 4)
                if o2:
                    second_sem[(par, o2)] = sem
                    send(
                        out2.at[layer, o2 - 1], in2.at[layer, o2 - 1],
                        rs_send.at[layer, sem], rs_recv.at[layer, sem], a2, o2,
                    )
                    sem += 1

        for par, a1, a2, out1, in1, out2, in2, own in sets:
            n2 = sizes[a2]
            for o in range(1, n2):
                at = second_sem[(par, o)]
                arrive(
                    in2.at[layer, o - 1], rs_send.at[layer, at], rs_recv.at[layer, at], a2, o
                )

            def add(q):
                acc = decode(in2[layer, 0, q])
                for o in range(2, n2):
                    acc = acc + decode(in2[layer, o - 1, q])
                acc = acc * back2 + own[q]
                zt = 2 * (q >> 2) + par
                z_out[layer, zt, q & 3] = encode(acc, scale3)
                z_own[zt, q & 3] = acc

            loop(zh * 4, add, 4)

        third = sem
        for o in range(1, nz):
            send(
                z_out.at[layer, other(Z, o)], z_in.at[layer, o - 1],
                rs_send.at[layer, third + o - 1], rs_recv.at[layer, third + o - 1], Z, o,
            )
        for o in range(1, nz):
            arrive(
                z_in.at[layer, o - 1],
                rs_send.at[layer, third + o - 1], rs_recv.at[layer, third + o - 1], Z, o,
            )
        for j in range(4):
            acc = decode(z_in[layer, 0, j])
            for o in range(2, nz):
                acc = acc + decode(z_in[layer, o - 1, j])
            acc = acc * back3 + z_own[me[Z], j]
            acc = acc + bias[layer : layer + 1, j * LANES : (j + 1) * LANES]
            done = jnp.clip(acc, 0.0, CEILING).astype(jnp.bfloat16)
            if layer + 1 < layers:
                put_acts(layer + 1, j, done)
            else:
                out[:, j * LANES : (j + 1) * LANES] = done

    for copy in started:
        copy.wait_send()


def local(sizes, images, tile_weights, tile_blocks, tile_count, bias):
    layers, slots, width, _ = tile_weights.shape
    rows = images.shape[0]
    nz, ny, nx = sizes[Z], sizes[Y], sizes[X]
    total = nz * ny * nx
    zh = nz // 2
    turned = jnp.transpose(tile_blocks, (0, 2, 1))
    if slots < LANES:
        turned = jnp.pad(turned, ((0, 0), (0, 0), (0, LANES - slots)), constant_values=0)
    counts = jnp.transpose(tile_count, (1, 0))
    block = (rows, LANES)
    n_ag = sum(len(part.messages()) for part in gather_parts(sizes))
    n_rs = 2 * (nx - 1) + 2 * (ny - 1) + nz - 1
    n_peer = nx - 1 + ny - 1

    def half(n1, n2):
        return [
            pltpu.VMEM((layers, n1 - 1, n2 * zh * 2, *block), jnp.int16),
            pltpu.VMEM((layers, n1 - 1, n2 * zh * 2 + 1, *block), jnp.int16),
            pltpu.VMEM((layers, n2 - 1, zh * 4, *block), jnp.int16),
            pltpu.VMEM((layers, n2 - 1, zh * 4, *block), jnp.int16),
            pltpu.VMEM((zh * 4, *block), jnp.float32),
        ]

    scratch = [
        pltpu.VMEM((layers, total * 4, *block), jnp.bfloat16),
        pltpu.VMEM((layers, slots, width, width), jnp.bfloat16),
        pltpu.VMEM((slots + 1, *block), jnp.int16),
        pltpu.VMEM((24, LANES), jnp.int32),
        pltpu.VMEM((n_peer, 8, LANES), jnp.int32),
        pltpu.SMEM((16, LANES), jnp.int32),
        pltpu.SMEM((n_peer, 8, LANES), jnp.int32),
        *half(nx, ny),
        *half(ny, nx),
        pltpu.VMEM((layers, nz, 4, *block), jnp.int16),
        pltpu.VMEM((layers, nz - 1, 4, *block), jnp.int16),
        pltpu.VMEM((nz, 4, *block), jnp.float32),
        pltpu.SemaphoreType.DMA((layers, n_ag)),
        pltpu.SemaphoreType.DMA((layers, n_ag)),
        pltpu.SemaphoreType.DMA((layers, n_rs)),
        pltpu.SemaphoreType.DMA((layers, n_rs)),
        pltpu.SemaphoreType.DMA((n_peer,)),
        pltpu.SemaphoreType.DMA((n_peer,)),
        pltpu.SemaphoreType.DMA((layers + 2,)),
    ]
    vmem = pl.BlockSpec(memory_space=pltpu.VMEM)
    return pl.pallas_call(
        functools.partial(kernel, sizes, layers, slots, rows),
        out_shape=jax.ShapeDtypeStruct(images.shape, images.dtype),
        in_specs=[
            vmem,
            pl.BlockSpec(memory_space=pltpu.HBM),
            vmem,
            pl.BlockSpec(memory_space=pltpu.SMEM),
            vmem,
        ],
        out_specs=vmem,
        scratch_shapes=scratch,
        compiler_params=pltpu.CompilerParams(
            collective_id=0, has_side_effects=True, vmem_limit_bytes=56 * 1024 * 1024
        ),
        name="layers",
    )(images, tile_weights, turned, counts, bias)


def solution(mesh):
    split = Mesh(
        mesh.devices.reshape(mesh.shape["batch"], 8, 4, 4),
        ("batch", "neuron_0", "neuron_1", "neuron_2"),
    )
    return sharded(split)


def sharded(split):
    sizes = {axis: split.shape[axis] for axis in AXES}
    in_specs = (
        P("batch", AXES),
        P(None, AXES, None, None),
        P(None, AXES, None),
        P(None, AXES),
        P(None, AXES),
    )
    return jax.shard_map(
        functools.partial(local, sizes), mesh=split, in_specs=in_specs,
        out_specs=P("batch", AXES), check_vma=False,
    )
```

```python
import functools

import jax
import jax.numpy as jnp
from jax import lax
from jax.experimental import pallas as pl
from jax.experimental.pallas import tpu as pltpu
from jax.sharding import Mesh
from jax.sharding import PartitionSpec as P

AXES = ("neuron_0", "neuron_1", "neuron_2")
Z, Y, X = AXES
CEILING = 32.0
WEIGHT_TOP = 0.375
MESH = pl.DeviceIdType.MESH
LANES = 128


def spot_a(sizes, z, y, x):
    return ((z * sizes[Y] + y) * sizes[X] + x) * 2


def spot_b(sizes, axis, me_z, outer, middle, z):
    total = sizes[Z] * sizes[Y] * sizes[X]
    other = Y if axis == X else X
    base = (2 if axis == X else 3) * total
    turned = (z - me_z + 2 + sizes[Z]) & (sizes[Z] - 1)
    return base + (outer * sizes[other] + middle) * sizes[Z] + turned


def encode(value, scale):
    coded = value * lax.rsqrt(jnp.abs(value) + 1e-30) * scale
    return jnp.round(coded).astype(jnp.int32).astype(jnp.int16)


def decode(coded):
    value = coded.astype(jnp.int32).astype(jnp.float32)
    return value * jnp.abs(value)


def kernel(sizes, layers, slots, rows, images, weights, blocks, count, bias, out, *scratch):
    (acts, held, products, table, peer, stab, speer, x_out, x_in, x_late, x_out2, x_in2, x_own,
     y_out, y_in, y_late, y_out2, y_in2, y_own, z_out, z_in, z_own,
     row_sem, z_sem, near_sem, mid_sem, last_sem, send_sem, first_sem, second_sem, third_sem,
     copy_sem) = scratch
    nz, ny, nx = sizes[Z], sizes[Y], sizes[X]
    me = {axis: lax.axis_index(axis) for axis in AXES}
    zh = nz // 2
    width = rows * 0 + LANES
    shift_x, shift_y = nx.bit_length() - 1, ny.bit_length() - 1
    total = nz * ny * nx
    top = WEIGHT_TOP * CEILING * width
    scale1 = 32700.0 / top ** 0.5
    scale2 = 32700.0 / (top * max(nx, ny)) ** 0.5
    scale3 = 32700.0 / (top * nx * ny) ** 0.5
    back1, back2, back3 = 1 / scale1**2, 1 / scale2**2, 1 / scale3**2

    def other(axis, step):
        return lax.rem(me[axis] + step + sizes[axis], sizes[axis])

    barrier = pltpu.get_barrier_semaphore()
    partners = [{Y: p, X: q} for p in range(ny) for q in range(nx) if p or q]
    partners += [{Z: o} for o in range(1, nz)]
    for steps in partners:
        pl.semaphore_signal(
            barrier, inc=1,
            device_id={axis: other(axis, o) for axis, o in steps.items()}, device_id_type=MESH,
        )

    weight_copies = [
        pltpu.make_async_copy(weights.at[l], held.at[l], copy_sem.at[l]) for l in range(layers)
    ]
    for copy in weight_copies:
        copy.start()

    own_spot = [
        spot_a(sizes, me[Z], me[Y], me[X]),
        spot_a(sizes, me[Z], me[Y], me[X]) + 1,
        spot_b(sizes, X, me[Z], me[X], me[Y], me[Z]),
        spot_b(sizes, Y, me[Z], me[Y], me[X], me[Z]),
    ]

    def put_acts(layer, j, value):
        acts[layer, own_spot[j]] = value

    for j in range(4):
        put_acts(0, j, images[:, j * LANES : (j + 1) * LANES])

    lane = lax.broadcasted_iota(jnp.int32, (1, LANES), 1)
    slot = lax.broadcasted_iota(jnp.int32, (LANES, LANES), 0)
    flat = jnp.concatenate(
        [blocks[0], blocks[1], jnp.zeros((4, LANES), jnp.int32)], axis=0
    )
    upright = jnp.transpose(flat)
    dx = lane & (nx - 1)
    dy = (lane >> shift_x) & (ny - 1)
    dz = lane >> (shift_x + shift_y)
    second = jnp.where((dz & 1) == 0, dy, dx)
    groups = 2 if zh > 1 else 1
    zg = zh // groups
    most = jnp.where((dz & 1) == 0, ny, nx) * zg
    place = (second * zg + (dz >> 1) % zg) * 2
    blank = most * 2
    for l in range(layers):
        r = blocks[l, 0:1, :]
        j = r & 3
        rx = (r >> 2) & (nx - 1)
        ry = (r >> (2 + shift_x)) & (ny - 1)
        rz = r >> (2 + shift_x + shift_y)
        spot = jnp.where(
            j < 2,
            spot_a(sizes, rz, ry, rx) + j,
            jnp.where(
                j == 2,
                spot_b(sizes, X, me[Z], rx, ry, rz),
                spot_b(sizes, Y, me[Z], ry, rx, rz),
            ),
        )
        table[l : l + 1, :] = spot
        key = jnp.where(slot < count[0, l], slot + 1, 0)
        col = upright[:, 2 * l + 1 : 2 * l + 2]
        before = jnp.zeros((1, LANES), jnp.int32)
        ranked = [jnp.zeros((1, LANES), jnp.int32) for _ in range(2)]
        for j in range(4):
            found = jnp.sum(jnp.where(col == lane * 4 + j, key, 0), axis=0, keepdims=True)
            live = found > 0
            table[8 + 4 * l + j : 9 + 4 * l + j, :] = jnp.where(live, found - 1, slots)
            table[16 + 4 * l + j : 17 + 4 * l + j, :] = jnp.where(live, place + before, blank)
            for k in range(2):
                ranked[k] = ranked[k] + jnp.where(before == k, found, 0)
            before = before + live.astype(jnp.int32)
        for k in range(2):
            table[2 + 2 * l + k : 3 + 2 * l + k, :] = jnp.where(
                ranked[k] > 0, ranked[k] - 1, slots
            )
    own_table = pltpu.make_async_copy(table.at[pl.ds(0, 16)], stab, copy_sem.at[layers])
    own_table.start()

    nothing = jnp.zeros((rows, LANES), jnp.int16)
    products[slots] = nothing
    for buffer in (x_in, x_late, y_in, y_late):
        for l in range(layers):
            for o in range(buffer.shape[1]):
                buffer[l, o, buffer.shape[2] - 1] = nothing

    pl.semaphore_wait(barrier, len(partners))

    def remote(src, dst, send, recv, steps):
        return pltpu.make_async_remote_copy(
            src_ref=src, dst_ref=dst, send_sem=send, recv_sem=recv,
            device_id={axis: other(axis, step) for axis, step in steps.items()},
            device_id_type=MESH,
        )

    def send(src, dst, send, recv, steps):
        remote(src, dst, send, recv, steps).start()

    def arrive(ref, recv):
        pltpu.make_async_copy(ref, ref, recv).wait()

    def gather(layer):
        def view(first, size):
            return acts.at[layer, pl.ds(first, size)]

        def share(first, size, recv, steps):
            send(view(first, size), view(first, size), send_sem.at[0], recv, steps)

        rows_by_distance = [0]
        for o in range(1, ny // 2 + 1):
            rows_by_distance += [o] if 2 * o == ny else [o, ny - o]
        for rel in rows_by_distance:
            for o in range(nx):
                if rel or o:
                    steps = {Y: rel, X: o} if rel else {X: o}
                    share(own_spot[0], 2, row_sem.at[rel], steps)
        near = min(5, nz)
        for axis, at in ((X, 2), (Y, 3)):
            for o in sorted(range(1, nz), key=lambda o: min(o, nz - o)):
                turned = (nz - o + 2) % nz
                base = own_spot[at] - (2 % nz)
                group = 0 if turned < near else 1
                send(
                    view(own_spot[at], 1), view(base + turned, 1), send_sem.at[0],
                    near_sem.at[2 * (at - 2) + group], {Z: o},
                )

        half = ny // 2
        tops = nz // 2

        def z_index(step, rel, way):
            if step > tops:
                return None
            if 2 * step == nz and (rows_by_distance.index(rel) % 2 == 0) != (way == 1):
                return None
            return ((step - 1) * ny + rel) * 2 + (way < 0)

        def z_view(far, rel, way):
            return spot_a(sizes, other(Z, -way * far), other(Y, -rel), 0)

        def z_go(step, rel, way):
            n = z_index(step, rel, way)
            if n is not None:
                share(z_view(step - 1, rel, way), 2 * nx, z_sem.at[n], {Z: way})

        def z_come(step, rel, way):
            n = z_index(step, rel, way)
            if n is not None:
                arrive(view(z_view(step, rel, way), 2 * nx), z_sem.at[n])
                z_go(step + 1, rel, way)

        def row(rel):
            units = nx if rel else nx - 1
            arrive(view(spot_a(sizes, me[Z], other(Y, -rel), 0), 2 * units), row_sem.at[rel])
            for way in (1, -1):
                z_go(1, rel, way)

        spans = [(0, near)] + ([(near, nz - near)] if nz > near else [])

        def chunk(axis, middle, group):
            first, size = spans[group]
            other_axis = Y if axis == X else X
            total = nz * ny * nx
            base = (2 if axis == X else 3) * total
            return base + (me[axis] * sizes[other_axis] + middle) * nz + first, size

        def last(axis, rel, group):
            other_axis = Y if axis == X else X
            first, size = chunk(axis, other(other_axis, -rel), group)
            for o in range(1, sizes[axis]):
                share(first, size, last_sem.at[int(axis == Y)], {axis: o})

        def lines(axis, group):
            at = 0 if axis == X else 1
            other_axis = Y if axis == X else X
            first, size = chunk(axis, me[other_axis], group)
            came = size - 1 if group == 0 else size
            if came:
                arrive(view(first, came), near_sem.at[2 * at + group])
            for o in range(1, sizes[other_axis]):
                share(first, size, mid_sem.at[mid(at, group, o)], {other_axis: o})
            last(axis, 0, group)

        def mid(at, group, o):
            return (at * 2 + group) * (max(nx, ny) - 1) + o - 1

        def middle(axis, group, o):
            at = 0 if axis == X else 1
            other_axis = Y if axis == X else X
            first, size = chunk(axis, other(other_axis, -o), group)
            arrive(view(first, size), mid_sem.at[mid(at, group, o)])
            last(axis, o, group)

        both = ((X, ny), (Y, nx))
        row(0)
        for axis, _ in both:
            lines(axis, 0)
        for rel in rows_by_distance[1:]:
            row(rel)
        if len(spans) > 1:
            for axis, _ in both:
                lines(axis, 1)
        steps = [(step, rel) for step in range(1, tops + 1) for rel in rows_by_distance]
        jobs = [
            (axis, group, o)
            for group in range(len(spans))
            for o in range(1, max(nx, ny))
            for axis, n in both
            if o < n
        ]
        for at, (step, rel) in enumerate(steps):
            for way in (1, -1):
                z_come(step, rel, way)
            if at >= 1:
                for job in jobs[:2]:
                    middle(*job)
                jobs = jobs[2:]
        for job in jobs:
            middle(*job)
        for axis, n in both:
            total = nz * ny * nx
            base = (2 if axis == X else 3) * total
            arrive(view(base, total - total // sizes[axis]), last_sem.at[int(axis == Y)])

    sets = [
        (0, X, Y, x_out, (x_in, x_late), x_out2, x_in2, x_own),
        (1, Y, X, y_out, (y_in, y_late), y_out2, y_in2, y_own),
    ]
    n_peer = [0, nx - 1]
    for par, a1, *_ in sets:
        for o in range(1, sizes[a1]):
            n = n_peer[par] + o - 1
            send(table.at[pl.ds(16, 8)], peer.at[n], send_sem.at[1], copy_sem.at[layers + 2], {a1: o})
    all_peers = n_peer[1] + ny - 1

    def device_of(par, zi, c1, c2):
        y, x = (c2, c1) if par == 0 else (c1, c2)
        return ((2 * zi + par) * ny + y) * nx + x

    def loop(length, body, unroll):
        unroll = min(unroll, length)

        @pl.loop(0, length // unroll)
        def _(at):
            for u in range(unroll):
                body(at * unroll + u)

    for layer in range(layers):
        gather(layer)
        if layer == 0:
            own_table.wait()
            arrive(peer, copy_sem.at[layers + 2])
            arrive(peer, send_sem.at[1])
            peer_table = pltpu.make_async_copy(peer, speer, copy_sem.at[layers + 1])
            peer_table.start()
        weight_copies[layer].wait()

        def multiply(s):
            got = jnp.dot(
                acts[layer, stab[layer, s]], held[layer, s], preferred_element_type=jnp.float32
            )
            products[s] = encode(got, scale1)

        loop(slots, multiply, 16)
        if layer == 0:
            peer_table.wait()

        tops = max(nx, ny)

        def first_at(par, group, o):
            return first_sem.at[(par * groups + group) * (tops - 1) + o - 1]

        def second_at(par, group, o):
            return second_sem.at[(par * groups + group) * (tops - 1) + o - 1]

        for group in range(groups):
            for o in range(1, tops):
                for par, a1, a2, out1, in1, *_ in sets:
                    if o >= sizes[a1]:
                        continue
                    target = other(a1, o)
                    span = sizes[a2] * zg * 2

                    def pack(p):
                        q = p >> 1
                        d = device_of(par, group * zg + q % zg, target, q // zg)
                        out1[layer, o - 1, group * span + p] = products[
                            stab[2 + 2 * layer + (p & 1), d]
                        ]

                    loop(span, pack, 8)
                    send(
                        out1.at[layer, o - 1, pl.ds(group * span, span)],
                        in1[group].at[layer, o - 1, pl.ds(0, span)],
                        send_sem.at[2 + par], first_at(par, group, o), {a1: o},
                    )

        for group in range(groups):
            for par, a1, a2, out1, in1, out2, in2, own in sets:
                n1, n2 = sizes[a1], sizes[a2]
                span = n2 * zg * 2
                for o in range(1, n1):
                    arrive(in1[group].at[layer, o - 1, pl.ds(0, span)], first_at(par, group, o))
                for o2 in list(range(1, n2)) + [0]:
                    target = other(a2, o2)

                    def add(at):
                        q = group * zg * 4 + at
                        j = q & 3
                        d = device_of(par, q >> 2, me[a1], target)
                        acc = decode(products[stab[8 + 4 * layer + j, d]])
                        for o in range(1, n1):
                            n = n_peer[par] + o - 1
                            acc = acc + decode(in1[group][layer, o - 1, speer[n, 4 * layer + j, d]])
                        acc = acc * back1
                        if o2:
                            out2[layer, o2 - 1, q] = encode(acc, scale2)
                        else:
                            own[q] = acc

                    loop(zg * 4, add, 4)
                    if o2:
                        part = pl.ds(group * zg * 4, zg * 4)
                        send(
                            out2.at[layer, o2 - 1, part], in2.at[layer, o2 - 1, part],
                            send_sem.at[4 + par], second_at(par, group, o2), {a2: o2},
                        )

        for group in range(groups):
            for par, a1, a2, out1, in1, out2, in2, own in sets:
                n2 = sizes[a2]
                for o in range(1, n2):
                    arrive(
                        in2.at[layer, o - 1, pl.ds(group * zg * 4, zg * 4)],
                        second_at(par, group, o),
                    )

                def add(at):
                    q = group * zg * 4 + at
                    acc = decode(in2[layer, 0, q])
                    for o in range(2, n2):
                        acc = acc + decode(in2[layer, o - 1, q])
                    acc = acc * back2 + own[q]
                    zt = 2 * (q >> 2) + par
                    z_out[layer, zt, q & 3] = encode(acc, scale3)
                    z_own[zt, q & 3] = acc

                loop(zg * 4, add, 4)
                for zi in range(group * zg, group * zg + zg):
                    zt = 2 * zi + par

                    @pl.when(me[Z] != zt)
                    def _():
                        pltpu.make_async_remote_copy(
                            src_ref=z_out.at[layer, zt], dst_ref=z_in.at[layer, me[Z]],
                            send_sem=send_sem.at[6], recv_sem=third_sem.at[0],
                            device_id={Z: zt}, device_id_type=MESH,
                        ).start()

        arrive(z_in.at[layer, pl.ds(0, nz - 1)], third_sem.at[0])
        for j in range(4):
            acc = decode(z_in[layer, other(Z, 1), j])
            for o in range(2, nz):
                acc = acc + decode(z_in[layer, other(Z, o), j])
            acc = acc * back3 + z_own[me[Z], j]
            acc = acc + bias[layer : layer + 1, j * LANES : (j + 1) * LANES]
            done = jnp.clip(acc, 0.0, CEILING).astype(jnp.bfloat16)
            if layer + 1 < layers:
                put_acts(layer + 1, j, done)
            else:
                out[:, j * LANES : (j + 1) * LANES] = done

        arrive(acts.at[layer, pl.ds(0, total * 4 - 4)], send_sem.at[0])
        for par, a1, a2, out1, in1, out2, *_ in sets:
            arrive(out1.at[layer], send_sem.at[2 + par])
            arrive(out2.at[layer], send_sem.at[4 + par])
        arrive(z_out.at[layer, pl.ds(0, nz - 1)], send_sem.at[6])


def local(sizes, images, tile_weights, tile_blocks, tile_count, bias):
    layers, slots, width, _ = tile_weights.shape
    rows = images.shape[0]
    nz, ny, nx = sizes[Z], sizes[Y], sizes[X]
    total = nz * ny * nx
    zh = nz // 2
    turned = jnp.transpose(tile_blocks, (0, 2, 1))
    if slots < LANES:
        turned = jnp.pad(turned, ((0, 0), (0, 0), (0, LANES - slots)), constant_values=0)
    counts = jnp.transpose(tile_count, (1, 0))
    block = (rows, LANES)
    groups = 2 if zh > 1 else 1
    zg = zh // groups
    per_set = groups * (max(nx, ny) - 1)
    n_peer = nx - 1 + ny - 1

    def half(n1, n2):
        return [
            pltpu.VMEM((layers, n1 - 1, n2 * zh * 2, *block), jnp.int16),
            pltpu.VMEM((layers, n1 - 1, n2 * zg * 2 + 1, *block), jnp.int16),
            pltpu.VMEM((layers, n1 - 1, n2 * zg * 2 + 1, *block), jnp.int16),
            pltpu.VMEM((layers, n2 - 1, zh * 4, *block), jnp.int16),
            pltpu.VMEM((layers, n2 - 1, zh * 4, *block), jnp.int16),
            pltpu.VMEM((zh * 4, *block), jnp.float32),
        ]

    scratch = [
        pltpu.VMEM((layers, total * 4, *block), jnp.bfloat16),
        pltpu.VMEM((layers, slots, width, width), jnp.bfloat16),
        pltpu.VMEM((slots + 1, *block), jnp.int16),
        pltpu.VMEM((24, LANES), jnp.int32),
        pltpu.VMEM((n_peer, 8, LANES), jnp.int32),
        pltpu.SMEM((16, LANES), jnp.int32),
        pltpu.SMEM((n_peer, 8, LANES), jnp.int32),
        *half(nx, ny),
        *half(ny, nx),
        pltpu.VMEM((layers, nz, 4, *block), jnp.int16),
        pltpu.VMEM((layers, nz, 4, *block), jnp.int16),
        pltpu.VMEM((nz, 4, *block), jnp.float32),
        pltpu.SemaphoreType.DMA((ny,)),
        pltpu.SemaphoreType.DMA((nz // 2 * ny * 2,)),
        pltpu.SemaphoreType.DMA((4,)),
        pltpu.SemaphoreType.DMA((4 * (max(nx, ny) - 1),)),
        pltpu.SemaphoreType.DMA((2,)),
        pltpu.SemaphoreType.DMA((7,)),
        pltpu.SemaphoreType.DMA((2 * per_set,)),
        pltpu.SemaphoreType.DMA((2 * per_set,)),
        pltpu.SemaphoreType.DMA((1,)),
        pltpu.SemaphoreType.DMA((layers + 3,)),
    ]
    vmem = pl.BlockSpec(memory_space=pltpu.VMEM)
    return pl.pallas_call(
        functools.partial(kernel, sizes, layers, slots, rows),
        out_shape=jax.ShapeDtypeStruct(images.shape, images.dtype),
        in_specs=[
            vmem,
            pl.BlockSpec(memory_space=pltpu.HBM),
            vmem,
            pl.BlockSpec(memory_space=pltpu.SMEM),
            vmem,
        ],
        out_specs=vmem,
        scratch_shapes=scratch,
        compiler_params=pltpu.CompilerParams(
            collective_id=0, has_side_effects=True, vmem_limit_bytes=56 * 1024 * 1024
        ),
        name="layers",
    )(images, tile_weights, turned, counts, bias)


def solution(mesh):
    split = Mesh(
        mesh.devices.reshape(mesh.shape["batch"], 8, 4, 4),
        ("batch", "neuron_0", "neuron_1", "neuron_2"),
    )
    return sharded(split)


def sharded(split):
    sizes = {axis: split.shape[axis] for axis in AXES}
    in_specs = (
        P("batch", AXES),
        P(None, AXES, None, None),
        P(None, AXES, None),
        P(None, AXES),
        P(None, AXES),
    )
    return jax.shard_map(
        functools.partial(local, sizes), mesh=split, in_specs=in_specs,
        out_specs=P("batch", AXES), check_vma=False,
    )
```

```python
import functools

import jax
import jax.numpy as jnp
from jax import lax
from jax.experimental import pallas as pl
from jax.experimental.pallas import tpu as pltpu
from jax.sharding import Mesh
from jax.sharding import PartitionSpec as P

AXES = ("neuron_0", "neuron_1", "neuron_2")
Z, Y, X = AXES
CEILING = 32.0
WEIGHT_TOP = 0.375
MESH = pl.DeviceIdType.MESH
LANES = 128


SHARES = ((1, 2, 1), (1, 1, 2))


def spot_a(sizes, shares, z, y, x):
    return ((z * sizes[Y] + y) * sizes[X] + x) * shares[0]


def base_of(sizes, shares, axis):
    return sizes[Z] * sizes[Y] * sizes[X] * (shares[0] + (shares[1] if axis == Y else 0))


def share_of(shares, axis):
    return shares[1] if axis == X else shares[2]


def spot_b(sizes, shares, axis, me_z, outer, middle, z):
    other = Y if axis == X else X
    turned = (z - me_z + 2 + sizes[Z]) & (sizes[Z] - 1)
    spot = (outer * sizes[other] + middle) * sizes[Z] + turned
    return base_of(sizes, shares, axis) + spot * share_of(shares, axis)


GROUPS = 4


def groups_of(zh):
    return min(GROUPS, zh)


def encode(value, scale):
    coded = value * lax.rsqrt(jnp.abs(value) + 1e-30) * scale
    return jnp.round(coded).astype(jnp.int32).astype(jnp.int16)


def decode(coded):
    value = coded.astype(jnp.int32).astype(jnp.float32)
    return value * jnp.abs(value)


def kernel(sizes, layers, slots, rows, images, weights, blocks, count, bias, out, *scratch):
    (acts, held, products, table, peer, stab, speer, x_out, x_out2, x_in2, x_own,
     y_out, y_out2, y_in2, y_own, z_out, z_in, z_own,
     row_sem, z_sem, near_sem, mid_sem, last_sem, send_sem, first_sem, second_sem, third_sem,
     copy_sem, *late) = scratch
    nz, ny, nx = sizes[Z], sizes[Y], sizes[X]
    me = {axis: lax.axis_index(axis) for axis in AXES}
    zh = nz // 2
    groups = groups_of(zh)
    zg = zh // groups
    x_in, y_in = late[:groups], late[groups:]
    shift_x, shift_y = nx.bit_length() - 1, ny.bit_length() - 1
    total = nz * ny * nx
    top = WEIGHT_TOP * CEILING * LANES
    scale1 = 32700.0 / top ** 0.5
    scale2 = 32700.0 / (top * max(nx, ny)) ** 0.5
    scale3 = 32700.0 / (top * nx * ny) ** 0.5
    back1, back2, back3 = 1 / scale1**2, 1 / scale2**2, 1 / scale3**2

    def other(axis, step):
        return lax.rem(me[axis] + step + sizes[axis], sizes[axis])

    barrier = pltpu.get_barrier_semaphore()
    partners = [{Y: p, X: q} for p in range(ny) for q in range(nx) if p or q]
    partners += [{Z: o} for o in range(1, nz)]
    for steps in partners:
        pl.semaphore_signal(
            barrier, inc=1,
            device_id={axis: other(axis, o) for axis, o in steps.items()}, device_id_type=MESH,
        )

    weight_copies = [
        pltpu.make_async_copy(weights.at[l], held.at[l], copy_sem.at[l]) for l in range(layers)
    ]
    for copy in weight_copies:
        copy.start()

    core = lax.axis_index("batch")

    def own_spots(shares):
        first_a = spot_a(sizes, shares, me[Z], me[Y], me[X])
        first_b = spot_b(sizes, shares, X, me[Z], me[X], me[Y], me[Z])
        first_c = spot_b(sizes, shares, Y, me[Z], me[Y], me[X], me[Z])
        return [
            first + at
            for first, share in zip((first_a, first_b, first_c), shares)
            for at in range(share)
        ]

    both_spots = [own_spots(shares) for shares in SHARES]
    own_spot = [p + core * (q - p) for p, q in zip(*both_spots)]

    def put_acts(layer, j, value):
        acts[layer, own_spot[j]] = value

    for j in range(4):
        put_acts(0, j, images[:, j * LANES : (j + 1) * LANES])

    lane = lax.broadcasted_iota(jnp.int32, (1, LANES), 1)
    slot = lax.broadcasted_iota(jnp.int32, (LANES, LANES), 0)
    flat = jnp.concatenate(
        [blocks[0], blocks[1], jnp.zeros((4, LANES), jnp.int32)], axis=0
    )
    upright = jnp.transpose(flat)
    dx = lane & (nx - 1)
    dy = (lane >> shift_x) & (ny - 1)
    dz = lane >> (shift_x + shift_y)
    second = jnp.where((dz & 1) == 0, dy, dx)
    most = jnp.where((dz & 1) == 0, ny, nx) * zg
    place = (second * zg + (dz >> 1) % zg) * 2
    blank = most * 2
    for l in range(layers):
        r = blocks[l, 0:1, :]
        j = r & 3
        rx = (r >> 2) & (nx - 1)
        ry = (r >> (2 + shift_x)) & (ny - 1)
        rz = r >> (2 + shift_x + shift_y)
        spots = []
        for shares in SHARES:
            in_a, in_b, in_c = (
                spot_a(sizes, shares, rz, ry, rx),
                spot_b(sizes, shares, X, me[Z], rx, ry, rz),
                spot_b(sizes, shares, Y, me[Z], ry, rx, rz),
            )
            to_b, to_c = shares[0], shares[0] + shares[1]
            spots.append(
                jnp.where(j < to_b, in_a + j, jnp.where(j < to_c, in_b + j - to_b, in_c + j - to_c))
            )
        spot = spots[0] + core * (spots[1] - spots[0])
        table[l : l + 1, :] = spot
        key = jnp.where(slot < count[0, l], slot + 1, 0)
        col = upright[:, 2 * l + 1 : 2 * l + 2]
        before = jnp.zeros((1, LANES), jnp.int32)
        ranked = [jnp.zeros((1, LANES), jnp.int32) for _ in range(2)]
        for j in range(4):
            found = jnp.sum(jnp.where(col == lane * 4 + j, key, 0), axis=0, keepdims=True)
            live = found > 0
            table[8 + 4 * l + j : 9 + 4 * l + j, :] = jnp.where(live, found - 1, slots)
            table[16 + 4 * l + j : 17 + 4 * l + j, :] = jnp.where(live, place + before, blank)
            for k in range(2):
                ranked[k] = ranked[k] + jnp.where(before == k, found, 0)
            before = before + live.astype(jnp.int32)
        for k in range(2):
            table[2 + 2 * l + k : 3 + 2 * l + k, :] = jnp.where(
                ranked[k] > 0, ranked[k] - 1, slots
            )
    own_table = pltpu.make_async_copy(table.at[pl.ds(0, 16)], stab, copy_sem.at[layers])
    own_table.start()

    nothing = jnp.zeros((rows, LANES), jnp.int16)
    products[slots] = nothing
    for buffer in late:
        for l in range(layers):
            for o in range(buffer.shape[1]):
                buffer[l, o, buffer.shape[2] - 1] = nothing

    pl.semaphore_wait(barrier, len(partners))

    def remote(src, dst, send, recv, steps):
        return pltpu.make_async_remote_copy(
            src_ref=src, dst_ref=dst, send_sem=send, recv_sem=recv,
            device_id={axis: other(axis, step) for axis, step in steps.items()},
            device_id_type=MESH,
        )

    def send(src, dst, send, recv, steps):
        remote(src, dst, send, recv, steps).start()

    def arrive(ref, recv):
        pltpu.make_async_copy(ref, ref, recv).wait()

    def gather(layer, shares):
        own = own_spots(shares)
        starts = (own[0], own[shares[0]], own[shares[0] + shares[1]])

        def view(first, size):
            return acts.at[layer, pl.ds(first, size)]

        def share(first, size, recv, steps):
            send(view(first, size), view(first, size), send_sem.at[0], recv, steps)

        rows_by_distance = [0]
        for o in range(1, ny // 2 + 1):
            rows_by_distance += [o] if 2 * o == ny else [o, ny - o]
        for rel in rows_by_distance:
            for o in range(nx):
                if rel or o:
                    steps = {Y: rel, X: o} if rel else {X: o}
                    share(starts[0], shares[0], row_sem.at[rel], steps)
        near = min(5, nz)
        for axis, at in ((X, 0), (Y, 1)):
            width = share_of(shares, axis)
            for o in sorted(range(1, nz), key=lambda o: min(o, nz - o)):
                turned = (nz - o + 2) % nz
                base = starts[1 + at] - (2 % nz) * width
                group = 0 if turned < near else 1
                send(
                    view(starts[1 + at], width), view(base + turned * width, width),
                    send_sem.at[0], near_sem.at[2 * at + group], {Z: o},
                )

        half = ny // 2
        tops = nz // 2

        def z_index(step, rel, way):
            if step > tops:
                return None
            if 2 * step == nz and (rows_by_distance.index(rel) % 2 == 0) != (way == 1):
                return None
            return ((step - 1) * ny + rel) * 2 + (way < 0)

        def z_view(far, rel, way):
            return spot_a(sizes, shares, other(Z, -way * far), other(Y, -rel), 0)

        def z_go(step, rel, way):
            n = z_index(step, rel, way)
            if n is not None:
                share(z_view(step - 1, rel, way), shares[0] * nx, z_sem.at[n], {Z: way})

        def z_come(step, rel, way):
            n = z_index(step, rel, way)
            if n is not None:
                arrive(view(z_view(step, rel, way), shares[0] * nx), z_sem.at[n])
                z_go(step + 1, rel, way)

        def row(rel):
            units = nx if rel else nx - 1
            first = spot_a(sizes, shares, me[Z], other(Y, -rel), 0)
            arrive(view(first, shares[0] * units), row_sem.at[rel])
            for way in (1, -1):
                z_go(1, rel, way)

        spans = [(0, near)] + ([(near, nz - near)] if nz > near else [])

        def chunk(axis, middle, group):
            first, size = spans[group]
            other_axis = Y if axis == X else X
            width = share_of(shares, axis)
            spot = (me[axis] * sizes[other_axis] + middle) * nz + first
            return base_of(sizes, shares, axis) + spot * width, size * width

        def last(axis, rel, group):
            other_axis = Y if axis == X else X
            first, size = chunk(axis, other(other_axis, -rel), group)
            for o in range(1, sizes[axis]):
                share(first, size, last_sem.at[int(axis == Y)], {axis: o})

        def lines(axis, group):
            at = 0 if axis == X else 1
            other_axis = Y if axis == X else X
            first, size = chunk(axis, me[other_axis], group)
            came = size - share_of(shares, axis) if group == 0 else size
            if came:
                arrive(view(first, came), near_sem.at[2 * at + group])
            for o in range(1, sizes[other_axis]):
                share(first, size, mid_sem.at[mid(at, group, o)], {other_axis: o})
            last(axis, 0, group)

        def mid(at, group, o):
            return (at * 2 + group) * (max(nx, ny) - 1) + o - 1

        def middle(axis, group, o):
            at = 0 if axis == X else 1
            other_axis = Y if axis == X else X
            first, size = chunk(axis, other(other_axis, -o), group)
            arrive(view(first, size), mid_sem.at[mid(at, group, o)])
            last(axis, o, group)

        both = ((X, ny), (Y, nx))
        row(0)
        for axis, _ in both:
            lines(axis, 0)
        for rel in rows_by_distance[1:]:
            row(rel)
        if len(spans) > 1:
            for axis, _ in both:
                lines(axis, 1)
        steps = [(step, rel) for step in range(1, tops + 1) for rel in rows_by_distance]
        jobs = [
            (axis, group, o)
            for group in range(len(spans))
            for o in range(1, max(nx, ny))
            for axis, n in both
            if o < n
        ]
        for at, (step, rel) in enumerate(steps):
            for way in (1, -1):
                z_come(step, rel, way)
            if at >= 1:
                for job in jobs[:2]:
                    middle(*job)
                jobs = jobs[2:]
        for job in jobs:
            middle(*job)
        for axis, n in both:
            came = (total - total // sizes[axis]) * share_of(shares, axis)
            arrive(view(base_of(sizes, shares, axis), came), last_sem.at[int(axis == Y)])

    sets = [
        (0, X, Y, x_out, x_in, x_out2, x_in2, x_own),
        (1, Y, X, y_out, y_in, y_out2, y_in2, y_own),
    ]
    n_peer = [0, nx - 1]
    for par, a1, *_ in sets:
        for o in range(1, sizes[a1]):
            n = n_peer[par] + o - 1
            send(table.at[pl.ds(16, 8)], peer.at[n], send_sem.at[1], copy_sem.at[layers + 2], {a1: o})
    all_peers = n_peer[1] + ny - 1

    def device_of(par, zi, c1, c2):
        y, x = (c2, c1) if par == 0 else (c1, c2)
        return ((2 * zi + par) * ny + y) * nx + x

    def loop(length, body, unroll):
        unroll = min(unroll, length)

        @pl.loop(0, length // unroll)
        def _(at):
            for u in range(unroll):
                body(at * unroll + u)

    for layer in range(layers):
        for at, shares in enumerate(SHARES):

            @pl.when(core == at)
            def _(shares=shares):
                gather(layer, shares)

        if layer == 0:
            own_table.wait()
            arrive(peer, copy_sem.at[layers + 2])
            arrive(peer, send_sem.at[1])
            peer_table = pltpu.make_async_copy(peer, speer, copy_sem.at[layers + 1])
            peer_table.start()
        weight_copies[layer].wait()

        def multiply(s):
            got = jnp.dot(
                acts[layer, stab[layer, s]], held[layer, s], preferred_element_type=jnp.float32
            )
            products[s] = encode(got, scale1)

        loop(slots, multiply, 16)
        if layer == 0:
            peer_table.wait()

        tops = max(nx, ny)

        def first_at(par, group, o):
            return first_sem.at[(par * groups + group) * (tops - 1) + o - 1]

        def second_at(par, group, o):
            return second_sem.at[(par * groups + group) * (tops - 1) + o - 1]

        for group in range(groups):
            for o in range(1, tops):
                for par, a1, a2, out1, in1, *_ in sets:
                    if o >= sizes[a1]:
                        continue
                    target = other(a1, o)
                    span = sizes[a2] * zg * 2

                    def pack(p):
                        q = p >> 1
                        d = device_of(par, group * zg + q % zg, target, q // zg)
                        out1[layer, o - 1, group * span + p] = products[
                            stab[2 + 2 * layer + (p & 1), d]
                        ]

                    loop(span, pack, 8)
                    send(
                        out1.at[layer, o - 1, pl.ds(group * span, span)],
                        in1[group].at[layer, o - 1, pl.ds(0, span)],
                        send_sem.at[2 + par], first_at(par, group, o), {a1: o},
                    )

        for group in range(groups):
            for par, a1, a2, out1, in1, out2, in2, own in sets:
                n1, n2 = sizes[a1], sizes[a2]
                span = n2 * zg * 2
                for o in range(1, n1):
                    arrive(in1[group].at[layer, o - 1, pl.ds(0, span)], first_at(par, group, o))
                for o2 in list(range(1, n2)) + [0]:
                    target = other(a2, o2)

                    def add(at):
                        q = group * zg * 4 + at
                        j = q & 3
                        d = device_of(par, q >> 2, me[a1], target)
                        acc = decode(products[stab[8 + 4 * layer + j, d]])
                        for o in range(1, n1):
                            n = n_peer[par] + o - 1
                            acc = acc + decode(in1[group][layer, o - 1, speer[n, 4 * layer + j, d]])
                        acc = acc * back1
                        if o2:
                            out2[layer, o2 - 1, q] = encode(acc, scale2)
                        else:
                            own[q] = acc

                    loop(zg * 4, add, 4)
                    if o2:
                        part = pl.ds(group * zg * 4, zg * 4)
                        send(
                            out2.at[layer, o2 - 1, part], in2.at[layer, o2 - 1, part],
                            send_sem.at[4 + par], second_at(par, group, o2), {a2: o2},
                        )

        for group in range(groups):
            for par, a1, a2, out1, in1, out2, in2, own in sets:
                n2 = sizes[a2]
                for o in range(1, n2):
                    arrive(
                        in2.at[layer, o - 1, pl.ds(group * zg * 4, zg * 4)],
                        second_at(par, group, o),
                    )

                def add(at):
                    q = group * zg * 4 + at
                    acc = decode(in2[layer, 0, q])
                    for o in range(2, n2):
                        acc = acc + decode(in2[layer, o - 1, q])
                    acc = acc * back2 + own[q]
                    zt = 2 * (q >> 2) + par
                    z_out[layer, zt, q & 3] = encode(acc, scale3)
                    z_own[zt, q & 3] = acc

                loop(zg * 4, add, 4)
                for zi in range(group * zg, group * zg + zg):
                    zt = 2 * zi + par

                    @pl.when(me[Z] != zt)
                    def _():
                        pltpu.make_async_remote_copy(
                            src_ref=z_out.at[layer, zt], dst_ref=z_in.at[layer, me[Z]],
                            send_sem=send_sem.at[6], recv_sem=third_sem.at[0],
                            device_id={Z: zt}, device_id_type=MESH,
                        ).start()

        arrive(z_in.at[layer, pl.ds(0, nz - 1)], third_sem.at[0])
        for j in range(4):
            acc = decode(z_in[layer, other(Z, 1), j])
            for o in range(2, nz):
                acc = acc + decode(z_in[layer, other(Z, o), j])
            acc = acc * back3 + z_own[me[Z], j]
            acc = acc + bias[layer : layer + 1, j * LANES : (j + 1) * LANES]
            done = jnp.clip(acc, 0.0, CEILING).astype(jnp.bfloat16)
            if layer + 1 < layers:
                put_acts(layer + 1, j, done)
            else:
                out[:, j * LANES : (j + 1) * LANES] = done

        arrive(acts.at[layer, pl.ds(0, total * 4 - 4)], send_sem.at[0])
        for par, a1, a2, out1, in1, out2, *_ in sets:
            arrive(out1.at[layer], send_sem.at[2 + par])
            arrive(out2.at[layer], send_sem.at[4 + par])
        arrive(z_out.at[layer, pl.ds(0, nz - 1)], send_sem.at[6])


def local(sizes, images, tile_weights, tile_blocks, tile_count, bias):
    layers, slots, width, _ = tile_weights.shape
    rows = images.shape[0]
    nz, ny, nx = sizes[Z], sizes[Y], sizes[X]
    total = nz * ny * nx
    zh = nz // 2
    turned = jnp.transpose(tile_blocks, (0, 2, 1))
    if slots < LANES:
        turned = jnp.pad(turned, ((0, 0), (0, 0), (0, LANES - slots)), constant_values=0)
    counts = jnp.transpose(tile_count, (1, 0))
    block = (rows, LANES)
    groups = groups_of(zh)
    zg = zh // groups
    per_set = groups * (max(nx, ny) - 1)
    n_peer = nx - 1 + ny - 1

    def half(n1, n2):
        return [
            pltpu.VMEM((layers, n1 - 1, n2 * zh * 2, *block), jnp.int16),
            pltpu.VMEM((layers, n2 - 1, zh * 4, *block), jnp.int16),
            pltpu.VMEM((layers, n2 - 1, zh * 4, *block), jnp.int16),
            pltpu.VMEM((zh * 4, *block), jnp.float32),
        ]

    scratch = [
        pltpu.VMEM((layers, total * 4, *block), jnp.bfloat16),
        pltpu.VMEM((layers, slots, width, width), jnp.bfloat16),
        pltpu.VMEM((slots + 1, *block), jnp.int16),
        pltpu.VMEM((24, LANES), jnp.int32),
        pltpu.VMEM((n_peer, 8, LANES), jnp.int32),
        pltpu.SMEM((16, LANES), jnp.int32),
        pltpu.SMEM((n_peer, 8, LANES), jnp.int32),
        *half(nx, ny),
        *half(ny, nx),
        pltpu.VMEM((layers, nz, 4, *block), jnp.int16),
        pltpu.VMEM((layers, nz, 4, *block), jnp.int16),
        pltpu.VMEM((nz, 4, *block), jnp.float32),
        pltpu.SemaphoreType.DMA((ny,)),
        pltpu.SemaphoreType.DMA((nz // 2 * ny * 2,)),
        pltpu.SemaphoreType.DMA((4,)),
        pltpu.SemaphoreType.DMA((4 * (max(nx, ny) - 1),)),
        pltpu.SemaphoreType.DMA((2,)),
        pltpu.SemaphoreType.DMA((7,)),
        pltpu.SemaphoreType.DMA((2 * per_set,)),
        pltpu.SemaphoreType.DMA((2 * per_set,)),
        pltpu.SemaphoreType.DMA((1,)),
        pltpu.SemaphoreType.DMA((layers + 3,)),
        *[
            pltpu.VMEM((layers, n1 - 1, n2 * zg * 2 + 1, *block), jnp.int16)
            for n1, n2 in ((nx, ny), (ny, nx))
            for _ in range(groups)
        ],
    ]
    vmem = pl.BlockSpec(memory_space=pltpu.VMEM)
    return pl.pallas_call(
        functools.partial(kernel, sizes, layers, slots, rows),
        out_shape=jax.ShapeDtypeStruct(images.shape, images.dtype),
        in_specs=[
            vmem,
            pl.BlockSpec(memory_space=pltpu.HBM),
            vmem,
            pl.BlockSpec(memory_space=pltpu.SMEM),
            vmem,
        ],
        out_specs=vmem,
        scratch_shapes=scratch,
        compiler_params=pltpu.CompilerParams(
            collective_id=0, has_side_effects=True, vmem_limit_bytes=56 * 1024 * 1024
        ),
        name="layers",
    )(images, tile_weights, turned, counts, bias)


def solution(mesh):
    split = Mesh(
        mesh.devices.reshape(mesh.shape["batch"], 8, 4, 4),
        ("batch", "neuron_0", "neuron_1", "neuron_2"),
    )
    return sharded(split)


def sharded(split):
    sizes = {axis: split.shape[axis] for axis in AXES}
    in_specs = (
        P("batch", AXES),
        P(None, AXES, None, None),
        P(None, AXES, None),
        P(None, AXES),
        P(None, AXES),
    )
    return jax.shard_map(
        functools.partial(local, sizes), mesh=split, in_specs=in_specs,
        out_specs=P("batch", AXES), check_vma=False,
    )
```
